32 devices in a mesh: view: 8 (over z, y), tok: 2 (over x), obj: 2 (over core).
Axes of the slice: x: 2, y: 2, z: 4, core: 2. Of those that a mesh axis runs over, the one named last changes fastest.
Arguments:
- latents: bfloat16 [512, 8, 2, 1280], P('tok', 'view', 'obj'), parts along dimension 2, may hold values from -8 to 8
- query_weight: bfloat16 [1280, 1024], P(None, 'tok'), may hold values from -2 to 2
- key_weight: bfloat16 [1280, 1024], P(None, 'tok'), may hold values from -14 to 14
- value_weight: bfloat16 [1280, 1024], P(None, 'tok'), may hold values from -0.15625 to 0.15625
- output_weight: bfloat16 [1024, 1280], P('tok'), may hold values from -0.1875 to 0.1875
- value_units: bfloat16 [1280, 5120], P(None, 'tok'), may hold values from -0.15625 to 0.15625
- gate_units: bfloat16 [1280, 5120], P(None, 'tok'), may hold values from -0.15625 to 0.15625
- down_weight: bfloat16 [5120, 1280], P('tok'), may hold values from -0.078125 to 0.078125
Outputs:
- refined: bfloat16 [512, 8, 2, 1280], P('tok', 'view', 'obj'), parts along dimension 2
The draws below stay inside these ranges and needn't reach their ends.
There are 2 independent parts, one for each index of `obj`. The reference program is written for one: setup_inputs(seed, part) draws one part's arguments, and reference() takes and returns one part's arrays. A program takes and returns all parts, laid end to end along the dimension named above; an argument that names none is the same for every part. Nothing has to cross between parts.
All inputs are finite; a program needn't handle non-finite values.
Results may differ from the reference program's by a relative error of at most 0.012.
Values may be sent and summed in bfloat16 or wider, within the bound.
A program may use at most 128 MiB of HBM per device.

```python
import jax
import jax.numpy as jnp
from jax import lax

D = 1280
HS = 64
FF = 5120
HEADS = 16
LT = 512
BATCH = 1
VIEWS = 8
HD = 1024
N_TOK = 2


def base_matrix(key):
    drawn = jax.random.normal(jax.random.fold_in(key, 7), (D, HEADS * HS), jnp.float32)
    return jnp.clip(drawn, -4.5, 4.5) / D ** 0.5


def draw_query_weight(key, part):
    return (2.5 * base_matrix(key)).astype(jnp.bfloat16)


def draw_key_weight(key, part):
    drawn = jax.random.normal(jax.random.fold_in(key, 9), (D, HEADS * HS), jnp.float32)
    independent = jnp.clip(drawn, -4.5, 4.5) / D ** 0.5
    result = independent
    return result.astype(jnp.bfloat16)


def draw_latents(key, part):
    extent = (LT, VIEWS, BATCH, D)
    result = jnp.clip(jax.random.normal(jax.random.fold_in(key, 6), extent, jnp.float32), -6.0, 6.0)
    return result.astype(jnp.bfloat16)


def steps_of(stream_key, shape, cuts, low, high):
    level, own = 1.0, jax.random.fold_in(stream_key, 6)
    for position, blocks in cuts:
        steps = jnp.exp(jax.random.uniform(jax.random.fold_in(own, position), (blocks,), jnp.float32, low / len(cuts), high / len(cuts)))
        level = level * jnp.repeat(steps, shape[position] // blocks).reshape([-1 if axis == position else 1 for axis in range(len(shape))])
    return level


def centred(own_key, shape, scale, most, split=(), kind=jnp.bfloat16):
    loudness = steps_of(own_key, shape, split, -0.22, 0.18) if split else 1.0
    values = jax.random.normal(own_key, shape, jnp.float32) * scale * loudness
    return jnp.minimum(jnp.maximum(values, -most), most).astype(kind)


def setup_inputs(seed: int = 0, part: int = 0) -> dict:
    key_of = jax.random.split(jax.random.key(seed), 9)
    own_keys = jax.random.split(jax.random.fold_in(key_of[8], part), 9)
    return {
        "latents": draw_latents(jax.random.fold_in(jax.random.fold_in(key_of[8], part), 71), part),
        "query_weight": draw_query_weight(jax.random.fold_in(key_of[8], 71), part),
        "key_weight": draw_key_weight(jax.random.fold_in(key_of[8], 71), part),
        "value_weight": centred(key_of[3], (D, HD), D ** -0.5, 0.15625, ((1, 2),)),
        "output_weight": centred(key_of[4], (HD, D), HD ** -0.5, 0.1875, ((0, 2),)),
        "value_units": centred(key_of[5], (D, FF), D ** -0.5, 0.15625, ((1, 2),)),
        "gate_units": centred(key_of[6], (D, FF), D ** -0.5, 0.15625, ((1, 2),)),
        "down_weight": centred(key_of[7], (FF, D), FF ** -0.5, 0.078125, ((0, 2),)),
    }


epsilon = 1e-05

def normalize(stream):
    average = lax.optimization_barrier(jnp.mean(stream, -1, keepdims=True))
    centered = stream - average
    spread = lax.optimization_barrier(jnp.mean(centered * centered, -1, keepdims=True))
    return centered * lax.rsqrt(spread + epsilon)

def head_attention(triple):
    queries, key_block, value_block = triple
    length_all = queries.shape[0]
    block_rows = 512 if length_all % 512 == 0 else length_all
    factor = HS ** (-0.5)

    def one_block(picked):
        scores = jnp.dot(picked, key_block.T, preferred_element_type=jnp.float32) * factor
        highest = lax.optimization_barrier(jnp.max(scores, -1, keepdims=True))
        weights = jnp.exp(scores - highest)
        totals = lax.optimization_barrier(jnp.sum(weights, -1, keepdims=True))
        blended = jnp.dot(weights.astype(jnp.bfloat16), value_block, preferred_element_type=jnp.float32)
        return blended / totals
    shaped = queries.reshape(length_all // block_rows, block_rows, queries.shape[1])
    return lax.map(one_block, shaped).reshape(length_all, queries.shape[1])

def reference(latents, query_weight, key_weight, value_weight, output_weight, value_units, gate_units, down_weight):
    stream = latents.astype(jnp.float32)
    normed = normalize(stream).astype(jnp.bfloat16)
    queries = jnp.dot(normed, query_weight, preferred_element_type=jnp.float32).astype(jnp.bfloat16)
    keys_all = jnp.dot(normed, key_weight, preferred_element_type=jnp.float32).astype(jnp.bfloat16)
    values_all = jnp.dot(normed, value_weight, preferred_element_type=jnp.float32).astype(jnp.bfloat16)

    def to_heads(projected):
        flat = projected.reshape(LT * VIEWS, BATCH, HEADS, HS)
        return flat.transpose(1, 2, 0, 3).reshape(BATCH * HEADS, LT * VIEWS, HS)
    blended = lax.map(head_attention, (to_heads(queries), to_heads(keys_all), to_heads(values_all)))
    attended = blended.reshape(BATCH, HEADS, LT * VIEWS, HS).transpose(2, 0, 1, 3)
    attended = attended.reshape(LT, VIEWS, BATCH, HEADS * HS).astype(jnp.bfloat16)
    head_width = HEADS * HS // N_TOK

    def add_heads(counter, totals):
        offset = (counter * head_width).astype(jnp.int32)
        chosen = lax.dynamic_slice_in_dim(attended, offset, head_width, 3)
        rows_block = lax.dynamic_slice_in_dim(output_weight, offset, head_width, 0)
        partial_sum = jnp.dot(chosen, rows_block, preferred_element_type=jnp.float32)
        return totals + partial_sum.astype(jnp.bfloat16).astype(jnp.float32)
    attention_out = lax.fori_loop(0, N_TOK, add_heads, jnp.zeros(stream.shape, jnp.float32))
    middle = stream + attention_out
    normed_two = normalize(middle).astype(jnp.bfloat16)
    unit_width = FF // N_TOK

    def add_units(counter, totals):
        offset = (counter * unit_width).astype(jnp.int32)
        linear = jnp.dot(normed_two, lax.dynamic_slice_in_dim(value_units, offset, unit_width, 1), preferred_element_type=jnp.float32)
        gating = jnp.dot(normed_two, lax.dynamic_slice_in_dim(gate_units, offset, unit_width, 1), preferred_element_type=jnp.float32)
        hidden = (linear * jax.nn.gelu(gating)).astype(jnp.bfloat16)
        rows_block = lax.dynamic_slice_in_dim(down_weight, offset, unit_width, 0)
        partial_sum = jnp.dot(hidden, rows_block, preferred_element_type=jnp.float32)
        return totals + partial_sum.astype(jnp.bfloat16).astype(jnp.float32)
    feed_out = lax.fori_loop(0, N_TOK, add_units, jnp.zeros(stream.shape, jnp.float32))
    return (middle + feed_out).astype(jnp.bfloat16)
```

```python
import functools

import jax
import jax.numpy as jnp
from jax import lax
from jax.experimental import pallas as pl
from jax.experimental.pallas import tpu as pltpu
from jax.sharding import PartitionSpec as P

HS = 64
MESH = pl.DeviceIdType.MESH
VMEM = pl.BlockSpec(memory_space=pltpu.VMEM)
ANY = pl.BlockSpec(memory_space=pl.ANY)


epsilon = 1e-05


def passed_along(block, axis, distance):
    devices = range(lax.axis_size(axis))
    route = [((i - distance) % len(devices), i) for i in devices]
    return lax.ppermute(block, axis, route)


def normalize(stream):
    average = jnp.mean(stream, -1, keepdims=True)
    centered = stream - average
    spread = jnp.mean(centered * centered, -1, keepdims=True)
    return centered * lax.rsqrt(spread + epsilon)


def meet(axes):
    barrier = pltpu.get_barrier_semaphore()
    for peer in axes:
        pl.semaphore_signal(barrier, inc=1, device_id=peer, device_id_type=MESH)
    pl.semaphore_wait(barrier, len(axes))


def peers_of(axis, count):
    me = lax.axis_index(axis)
    return [lax.rem(me + d, count) for d in range(1, count)]


def post(sources, results, axis, count, send_sem, recv_sem, own_sem, scattered):
    me = lax.axis_index(axis)
    waits = []
    for number, (source, result) in enumerate(zip(sources, results)):
        for d in range(1, count):
            peer = lax.rem(me + d, count)
            sender = lax.rem(me - d + count, count)
            copy = pltpu.make_async_remote_copy(
                src_ref=source.at[peer] if scattered else source,
                dst_ref=result.at[me],
                send_sem=send_sem.at[number, d],
                recv_sem=recv_sem.at[number, d],
                device_id={axis: peer},
                device_id_type=MESH,
            )
            arrival = pltpu.make_async_remote_copy(
                src_ref=source.at[peer] if scattered else source,
                dst_ref=result.at[sender],
                send_sem=send_sem.at[number, d],
                recv_sem=recv_sem.at[number, d],
                device_id={axis: peer},
                device_id_type=MESH,
            )
            copy.start()
            waits.append(copy.wait_send)
            waits.append(arrival.wait_recv)
        own = pltpu.make_async_copy(
            source.at[me] if scattered else source, result.at[me], own_sem.at[number]
        )
        own.start()
        waits.append(own.wait)
    return waits


def token_kernel(count, scattered, x_ref, out_ref, send_sem, recv_sem, own_sem):
    meet([{"tok": p} for p in peers_of("tok", count)])
    for wait in post([x_ref], [out_ref], "tok", count, send_sem, recv_sem, own_sem, scattered):
        wait()


def over_tokens(x, count, scattered, number):
    block = x.shape[1:] if scattered else x.shape
    return pl.pallas_call(
        functools.partial(token_kernel, count, scattered),
        out_shape=jax.ShapeDtypeStruct((count,) + block, x.dtype),
        in_specs=[VMEM],
        out_specs=ANY,
        scratch_shapes=[
            pltpu.SemaphoreType.DMA((1, count)),
            pltpu.SemaphoreType.DMA((1, count)),
            pltpu.SemaphoreType.DMA((1,)),
        ],
        compiler_params=pltpu.CompilerParams(collective_id=number, has_side_effects=True),
        name=f"over_tokens_{number}",
    )(x)


def heads_kernel(views, toks, q, k, v, w, q_out, k_out, v_out, w_out, *sems):
    meet(
        [{"view": p} for p in peers_of("view", views)]
        + [{"tok": p} for p in peers_of("tok", toks)]
    )
    waits = post([q, k, v], [q_out, k_out, v_out], "view", views, *sems[:3], True)
    waits += post([w], [w_out], "tok", toks, *sems[3:], False)
    for wait in waits:
        wait()


def spread_heads(queries, keys, values, weight, views, toks):
    like = jax.ShapeDtypeStruct(queries.shape, queries.dtype)
    return pl.pallas_call(
        functools.partial(heads_kernel, views, toks),
        out_shape=(like, like, like, jax.ShapeDtypeStruct((toks,) + weight.shape, weight.dtype)),
        in_specs=[VMEM] * 4,
        out_specs=(ANY,) * 4,
        scratch_shapes=[
            pltpu.SemaphoreType.DMA((3, views)),
            pltpu.SemaphoreType.DMA((3, views)),
            pltpu.SemaphoreType.DMA((3,)),
            pltpu.SemaphoreType.DMA((1, toks)),
            pltpu.SemaphoreType.DMA((1, toks)),
            pltpu.SemaphoreType.DMA((1,)),
        ],
        compiler_params=pltpu.CompilerParams(collective_id=1, has_side_effects=True),
        name="spread_heads",
    )(queries, keys, values, weight)


def attention_kernel(
    views, toks, q_ref, k_ref, v_ref, out_ref, keys, staged, send_sem, recv_sem, own_sem
):
    view, tok = lax.axis_index("view"), lax.axis_index("tok")
    others = [
        (dv, dt) for dv in range(views) for dt in range(toks) if dv or dt
    ]
    meet(
        [
            {"view": lax.rem(view + dv, views), "tok": lax.rem(tok + dt, toks)}
            for dv, dt in others
        ]
    )
    rows = staged.shape[-1]
    length = k_ref.shape[-1]
    for block in range(views):
        keys[block] = k_ref[block].T

    def attend(target, half):
        q = q_ref[target, :, pl.ds(pl.multiple_of(half * rows, rows), rows)]
        highest = jnp.full((1, rows), -1e30, jnp.float32)
        totals = jnp.zeros((1, rows), jnp.float32)
        blended = jnp.zeros((HS, rows), jnp.float32)
        for block in range(views):
            scores = jnp.dot(keys[block], q, preferred_element_type=jnp.float32)
            newest = jnp.maximum(highest, jnp.max(scores, 0, keepdims=True))
            shrink = jnp.exp(highest - newest)
            weights = jnp.exp(scores - newest)
            totals = totals * shrink + jnp.sum(weights, 0, keepdims=True)
            blended = blended * shrink + jnp.dot(
                v_ref[block], weights.astype(jnp.bfloat16), preferred_element_type=jnp.float32
            )
            highest = newest
        return (blended / totals).astype(jnp.bfloat16)

    def copy_to(dv, dt):
        target, half = lax.rem(view + dv, views), lax.rem(tok + dt, toks)
        return pltpu.make_async_remote_copy(
            src_ref=staged.at[dv, dt],
            dst_ref=out_ref.at[tok, view],
            send_sem=send_sem.at[dv, dt],
            recv_sem=recv_sem.at[dv, dt],
            device_id={"view": target, "tok": half},
            device_id_type=MESH,
        )

    def one_view(dv, carry):
        for dt in range(toks):
            target, half = lax.rem(view + dv, views), lax.rem(tok + dt, toks)
            staged[dv, dt] = attend(target, half)
            copy_to(dv, dt).start()
        return carry

    lax.fori_loop(1, views, one_view, 0)
    for dt in list(range(1, toks)) + [0]:
        staged[0, dt] = attend(view, lax.rem(tok + dt, toks))
        if dt:
            copy_to(0, dt).start()
    own = pltpu.make_async_copy(staged.at[0, 0], out_ref.at[tok, view], own_sem)
    own.start()
    for dv, dt in others:
        copy_to(dv, dt).wait_send()
        pltpu.make_async_remote_copy(
            src_ref=staged.at[dv, dt],
            dst_ref=out_ref.at[
                lax.rem(tok - dt + toks, toks), lax.rem(view - dv + views, views)
            ],
            send_sem=send_sem.at[dv, dt],
            recv_sem=recv_sem.at[dv, dt],
            device_id={"view": view, "tok": tok},
            device_id_type=MESH,
        ).wait_recv()
    own.wait()


def attention(queries, keys, values, views, toks):
    length = queries.shape[-1]
    rows = length // toks
    return pl.pallas_call(
        functools.partial(attention_kernel, views, toks),
        out_shape=jax.ShapeDtypeStruct((toks, views, HS, rows), jnp.bfloat16),
        in_specs=[VMEM] * 3,
        out_specs=ANY,
        scratch_shapes=[
            pltpu.VMEM((views, length, HS), jnp.bfloat16),
            pltpu.VMEM((views, toks, HS, rows), jnp.bfloat16),
            pltpu.SemaphoreType.DMA((views, toks)),
            pltpu.SemaphoreType.DMA((views, toks)),
            pltpu.SemaphoreType.DMA,
        ],
        compiler_params=pltpu.CompilerParams(collective_id=2, has_side_effects=True),
        name="attention",
    )(queries, keys, values)


def by_heads(
    latents,
    query_weight,
    key_weight,
    value_weight,
    output_weight,
    value_units,
    gate_units,
    down_weight,
):
    toks, views = lax.axis_size("tok"), lax.axis_size("view")
    head_width = query_weight.shape[1]
    width = latents.shape[-1]
    stream = latents.reshape(-1, width).astype(jnp.float32)
    rows = stream.shape[0]
    normed = normalize(stream).astype(jnp.bfloat16)
    gathered = over_tokens(normed, toks, False, 0).reshape(toks * rows, width)

    def project(weight):
        return lax.dot_general(
            weight, gathered, (((0,), (1,)), ((), ())), preferred_element_type=jnp.float32
        )

    def heads(projected):
        return projected.astype(jnp.bfloat16).reshape(views, HS, toks * rows)

    queries = heads(project(query_weight) * HS ** (-0.5))
    keys, values = heads(project(key_weight)), heads(project(value_weight))
    queries, keys, values, full_output = spread_heads(
        queries, keys, values, output_weight, views, toks
    )
    attended = attention(queries, keys, values, views, toks).reshape(toks, head_width, rows)
    group_parts = jnp.einsum(
        "gcr,gcd->grd", attended, full_output, preferred_element_type=jnp.float32
    ).astype(jnp.bfloat16)
    middle = stream + jnp.sum(group_parts.astype(jnp.float32), 0)
    normed_two = normalize(middle).astype(jnp.bfloat16)
    gathered_two = over_tokens(normed_two, toks, False, 3).reshape(toks * rows, width)
    linear = jnp.dot(gathered_two, value_units, preferred_element_type=jnp.float32)
    gating = jnp.dot(gathered_two, gate_units, preferred_element_type=jnp.float32)
    hidden = (linear * jax.nn.gelu(gating)).astype(jnp.bfloat16)
    unit_part = jnp.dot(hidden, down_weight, preferred_element_type=jnp.float32)
    unit_part = unit_part.astype(jnp.bfloat16).reshape(toks, rows, width)
    parts = over_tokens(unit_part, toks, True, 4)
    refined = middle + jnp.sum(parts.astype(jnp.float32), 0)
    return refined.astype(jnp.bfloat16).reshape(latents.shape)


def by_ring(
    latents,
    query_weight,
    key_weight,
    value_weight,
    output_weight,
    value_units,
    gate_units,
    down_weight,
):
    stream = latents.astype(jnp.float32)
    normed = normalize(stream).astype(jnp.bfloat16)
    joined = jnp.concatenate([query_weight, key_weight, value_weight], 1)
    projected = jnp.dot(
        lax.all_gather(normed, "tok", axis=0, tiled=True),
        joined,
        preferred_element_type=jnp.float32,
    ).astype(jnp.bfloat16)
    head_width = query_weight.shape[1]
    queries = projected[..., :head_width]
    key_part = projected[..., head_width : 2 * head_width]
    value_part = projected[..., 2 * head_width :]
    length_all, local_views, objects = (queries.shape[0], queries.shape[1], queries.shape[2])
    head_count = head_width // HS
    query_rows = length_all * local_views
    queries_flat = queries.reshape(query_rows, objects, head_count, HS)
    factor = HS ** (-0.5)

    def attend(states, key_block, value_block):
        key_rows = key_block.shape[0]

        def one_view(counter, inner):
            highest, totals, blended = inner
            key_view = lax.dynamic_index_in_dim(key_block, counter, 1, keepdims=False).reshape(
                key_rows, objects, head_count, HS
            )
            value_view = lax.dynamic_index_in_dim(value_block, counter, 1, keepdims=False).reshape(
                key_rows, objects, head_count, HS
            )
            scores = (
                jnp.einsum(
                    "ibhe,jbhe->bhij", queries_flat, key_view, preferred_element_type=jnp.float32
                )
                * factor
            )
            newest = jnp.maximum(highest, jnp.max(scores, -1))
            shrink = jnp.exp(highest - newest)
            weights = jnp.exp(scores - newest[..., None])
            totals = totals * shrink + jnp.sum(weights, -1)
            update = jnp.einsum(
                "bhij,jbhe->bhie",
                weights.astype(jnp.bfloat16),
                value_view,
                preferred_element_type=jnp.float32,
            )
            blended = blended * shrink[..., None] + update
            return (newest, totals, blended)

        return lax.fori_loop(0, key_block.shape[1], one_view, states)

    start_state = (
        jnp.full((objects, head_count, query_rows), -1e30, jnp.float32),
        jnp.zeros((objects, head_count, query_rows), jnp.float32),
        jnp.zeros((objects, head_count, query_rows, HS), jnp.float32),
    )
    stacked = jnp.stack([key_part, value_part])
    states = attend(start_state, key_part, value_part)

    def rotate(counter, bundle):
        inner, buffer_kv = bundle
        buffer_kv = passed_along(buffer_kv, "view", 1)
        return (attend(inner, buffer_kv[0], buffer_kv[1]), buffer_kv)

    states, stacked = lax.fori_loop(0, lax.axis_size("view") - 1, rotate, (states, stacked))
    highest, totals, blended = states
    attended = (blended / totals[..., None]).transpose(2, 0, 1, 3)
    attended = attended.reshape(length_all, local_views, objects, head_width).astype(jnp.bfloat16)
    full_output = lax.all_gather(output_weight, "tok", axis=0, tiled=True)
    own_rows = lax.all_to_all(attended, "tok", split_axis=0, concat_axis=3, tiled=True)
    groups = lax.axis_size("tok")
    grouped = own_rows.reshape(
        own_rows.shape[0], own_rows.shape[1], own_rows.shape[2], groups, head_width
    )
    weight_groups = full_output.reshape(groups, head_width, full_output.shape[1])
    group_parts = jnp.einsum(
        "rvbgc,gcd->rvbgd", grouped, weight_groups, preferred_element_type=jnp.float32
    ).astype(jnp.bfloat16)
    attention_out = jnp.sum(group_parts.astype(jnp.float32), 3)
    middle = stream + attention_out
    normed_two = normalize(middle).astype(jnp.bfloat16)
    gathered = lax.all_gather(normed_two, "tok", axis=0, tiled=True)
    linear = jnp.dot(gathered, value_units, preferred_element_type=jnp.float32)
    gating = jnp.dot(gathered, gate_units, preferred_element_type=jnp.float32)
    hidden = (linear * jax.nn.gelu(gating)).astype(jnp.bfloat16)
    feed_out = lax.psum_scatter(
        jnp.dot(hidden, down_weight, preferred_element_type=jnp.float32).astype(jnp.bfloat16),
        "tok",
        scatter_dimension=0,
        tiled=True,
    ).astype(jnp.float32)
    return (middle + feed_out).astype(jnp.bfloat16)


def on_device(latents, query_weight, *weights):
    head_count = query_weight.shape[1] // HS
    one_each = latents.shape[1] == 1 and latents.shape[2] == 1
    if one_each and head_count == lax.axis_size("view"):
        return by_heads(latents, query_weight, *weights)
    return by_ring(latents, query_weight, *weights)


def solution(mesh):
    return jax.shard_map(
        on_device,
        mesh=mesh,
        in_specs=(
            P("tok", "view", "obj", None),
            P(None, "tok"),
            P(None, "tok"),
            P(None, "tok"),
            P("tok", None),
            P(None, "tok"),
            P(None, "tok"),
            P("tok", None),
        ),
        out_specs=P("tok", "view", "obj", None),
        check_vma=False,
    )
```

```python
import functools

import jax
import jax.numpy as jnp
from jax import lax
from jax.experimental import pallas as pl
from jax.experimental.pallas import tpu as pltpu
from jax.sharding import PartitionSpec as P

HS = 64
MESH = pl.DeviceIdType.MESH
VMEM = pl.BlockSpec(memory_space=pltpu.VMEM)
ANY = pl.BlockSpec(memory_space=pl.ANY)


epsilon = 1e-05


def passed_along(block, axis, distance):
    devices = range(lax.axis_size(axis))
    route = [((i - distance) % len(devices), i) for i in devices]
    return lax.ppermute(block, axis, route)


def normalize(stream):
    average = jnp.mean(stream, -1, keepdims=True)
    centered = stream - average
    spread = jnp.mean(centered * centered, -1, keepdims=True)
    return centered * lax.rsqrt(spread + epsilon)


def meet(axes):
    barrier = pltpu.get_barrier_semaphore()
    for peer in axes:
        pl.semaphore_signal(barrier, inc=1, device_id=peer, device_id_type=MESH)
    pl.semaphore_wait(barrier, len(axes))


def peers_of(axis, count):
    me = lax.axis_index(axis)
    return [lax.rem(me + d, count) for d in range(1, count)]


def post(sources, results, axis, count, send_sem, recv_sem, own_sem, scattered):
    me = lax.axis_index(axis)
    waits = []
    for number, (source, result) in enumerate(zip(sources, results)):
        for d in range(1, count):
            peer = lax.rem(me + d, count)
            sender = lax.rem(me - d + count, count)
            copy = pltpu.make_async_remote_copy(
                src_ref=source.at[peer] if scattered else source,
                dst_ref=result.at[me],
                send_sem=send_sem.at[number, d],
                recv_sem=recv_sem.at[number, d],
                device_id={axis: peer},
                device_id_type=MESH,
            )
            arrival = pltpu.make_async_remote_copy(
                src_ref=source.at[peer] if scattered else source,
                dst_ref=result.at[sender],
                send_sem=send_sem.at[number, d],
                recv_sem=recv_sem.at[number, d],
                device_id={axis: peer},
                device_id_type=MESH,
            )
            copy.start()
            waits.append(copy.wait_send)
            waits.append(arrival.wait_recv)
        own = pltpu.make_async_copy(
            source.at[me] if scattered else source, result.at[me], own_sem.at[number]
        )
        own.start()
        waits.append(own.wait)
    return waits


def token_kernel(count, scattered, x_ref, out_ref, send_sem, recv_sem, own_sem):
    meet([{"tok": p} for p in peers_of("tok", count)])
    for wait in post([x_ref], [out_ref], "tok", count, send_sem, recv_sem, own_sem, scattered):
        wait()


def over_tokens(x, count, scattered, number):
    block = x.shape[1:] if scattered else x.shape
    return pl.pallas_call(
        functools.partial(token_kernel, count, scattered),
        out_shape=jax.ShapeDtypeStruct((count,) + block, x.dtype),
        in_specs=[VMEM],
        out_specs=ANY,
        scratch_shapes=[
            pltpu.SemaphoreType.DMA((1, count)),
            pltpu.SemaphoreType.DMA((1, count)),
            pltpu.SemaphoreType.DMA((1,)),
        ],
        compiler_params=pltpu.CompilerParams(collective_id=number, has_side_effects=True),
        name=f"over_tokens_{number}",
    )(x)


def heads_kernel(views, toks, q, k, v, w, q_out, k_out, v_out, w_out, *sems):
    meet(
        [{"view": p} for p in peers_of("view", views)]
        + [{"tok": p} for p in peers_of("tok", toks)]
    )
    waits = post([q, k, v], [q_out, k_out, v_out], "view", views, *sems[:3], True)
    waits += post([w], [w_out], "tok", toks, *sems[3:], False)
    for wait in waits:
        wait()


def spread_heads(queries, keys, values, weight, views, toks):
    like = jax.ShapeDtypeStruct(queries.shape, queries.dtype)
    return pl.pallas_call(
        functools.partial(heads_kernel, views, toks),
        out_shape=(like, like, like, jax.ShapeDtypeStruct((toks,) + weight.shape, weight.dtype)),
        in_specs=[VMEM] * 4,
        out_specs=(ANY,) * 4,
        scratch_shapes=[
            pltpu.SemaphoreType.DMA((3, views)),
            pltpu.SemaphoreType.DMA((3, views)),
            pltpu.SemaphoreType.DMA((3,)),
            pltpu.SemaphoreType.DMA((1, toks)),
            pltpu.SemaphoreType.DMA((1, toks)),
            pltpu.SemaphoreType.DMA((1,)),
        ],
        compiler_params=pltpu.CompilerParams(collective_id=1, has_side_effects=True),
        name="spread_heads",
    )(queries, keys, values, weight)


def attention_kernel(
    views, toks, q_ref, k_ref, v_ref, out_ref, keys, scores, staged, send_sem, recv_sem, own_sem
):
    view, tok = lax.axis_index("view"), lax.axis_index("tok")
    others = [
        (dv, dt) for dv in range(views) for dt in range(toks) if dv or dt
    ]
    meet(
        [
            {"view": lax.rem(view + dv, views), "tok": lax.rem(tok + dt, toks)}
            for dv, dt in others
        ]
    )
    rows = staged.shape[-1]
    length = k_ref.shape[-1]
    for block in range(views):
        keys[block] = k_ref[block].T

    def attend(target):
        q = q_ref[target]
        highest = jnp.full((1, length), -1e30, jnp.float32)
        for block in range(views):
            found = jnp.dot(keys[block], q, preferred_element_type=jnp.float32)
            scores[block] = found
            highest = jnp.maximum(highest, jnp.max(found, 0, keepdims=True))
        totals = jnp.zeros((1, length), jnp.float32)
        blended = jnp.zeros((HS, length), jnp.float32)
        for block in range(views):
            weights = jnp.exp(scores[block] - highest)
            totals = totals + jnp.sum(weights, 0, keepdims=True)
            blended = blended + jnp.dot(
                v_ref[block], weights.astype(jnp.bfloat16), preferred_element_type=jnp.float32
            )
        return (blended / totals).astype(jnp.bfloat16)

    def stage(dv):
        attended = attend(lax.rem(view + dv, views))
        for half in range(toks):
            staged[dv, half] = attended[:, half * rows : (half + 1) * rows]

    def copy_to(dv, dt):
        target, half = lax.rem(view + dv, views), lax.rem(tok + dt, toks)
        return pltpu.make_async_remote_copy(
            src_ref=staged.at[dv, half],
            dst_ref=out_ref.at[tok, view],
            send_sem=send_sem.at[dv, dt],
            recv_sem=recv_sem.at[dv, dt],
            device_id={"view": target, "tok": half},
            device_id_type=MESH,
        )

    def one_view(dv, carry):
        stage(dv)
        for dt in range(toks):
            copy_to(dv, dt).start()
        return carry

    lax.fori_loop(1, views, one_view, 0)
    stage(0)
    for dt in range(1, toks):
        copy_to(0, dt).start()
    own = pltpu.make_async_copy(staged.at[0, tok], out_ref.at[tok, view], own_sem)
    own.start()
    for dv, dt in others:
        copy_to(dv, dt).wait_send()
        pltpu.make_async_remote_copy(
            src_ref=staged.at[dv, dt],
            dst_ref=out_ref.at[
                lax.rem(tok - dt + toks, toks), lax.rem(view - dv + views, views)
            ],
            send_sem=send_sem.at[dv, dt],
            recv_sem=recv_sem.at[dv, dt],
            device_id={"view": view, "tok": tok},
            device_id_type=MESH,
        ).wait_recv()
    own.wait()


def attention(queries, keys, values, views, toks):
    length = queries.shape[-1]
    rows = length // toks
    return pl.pallas_call(
        functools.partial(attention_kernel, views, toks),
        out_shape=jax.ShapeDtypeStruct((toks, views, HS, rows), jnp.bfloat16),
        in_specs=[VMEM] * 3,
        out_specs=ANY,
        scratch_shapes=[
            pltpu.VMEM((views, length, HS), jnp.bfloat16),
            pltpu.VMEM((views, length, length), jnp.float32),
            pltpu.VMEM((views, toks, HS, rows), jnp.bfloat16),
            pltpu.SemaphoreType.DMA((views, toks)),
            pltpu.SemaphoreType.DMA((views, toks)),
            pltpu.SemaphoreType.DMA,
        ],
        compiler_params=pltpu.CompilerParams(collective_id=2, has_side_effects=True),
        name="attention",
    )(queries, keys, values)


def by_heads(
    latents,
    query_weight,
    key_weight,
    value_weight,
    output_weight,
    value_units,
    gate_units,
    down_weight,
):
    toks, views = lax.axis_size("tok"), lax.axis_size("view")
    head_width = query_weight.shape[1]
    width = latents.shape[-1]
    stream = latents.reshape(-1, width).astype(jnp.float32)
    rows = stream.shape[0]
    normed = normalize(stream).astype(jnp.bfloat16)
    gathered = over_tokens(normed, toks, False, 0).reshape(toks * rows, width)

    def project(weight):
        return lax.dot_general(
            weight, gathered, (((0,), (1,)), ((), ())), preferred_element_type=jnp.float32
        )

    def heads(projected):
        return projected.astype(jnp.bfloat16).reshape(views, HS, toks * rows)

    queries = heads(project(query_weight) * HS ** (-0.5))
    keys, values = heads(project(key_weight)), heads(project(value_weight))
    queries, keys, values, full_output = spread_heads(
        queries, keys, values, output_weight, views, toks
    )
    attended = attention(queries, keys, values, views, toks).reshape(toks, head_width, rows)
    group_parts = jnp.einsum(
        "gcr,gcd->grd", attended, full_output, preferred_element_type=jnp.float32
    ).astype(jnp.bfloat16)
    middle = stream + jnp.sum(group_parts.astype(jnp.float32), 0)
    normed_two = normalize(middle).astype(jnp.bfloat16)

    def feed(block):
        linear = jnp.dot(block, value_units, preferred_element_type=jnp.float32)
        gating = jnp.dot(block, gate_units, preferred_element_type=jnp.float32)
        hidden = (linear * jax.nn.gelu(gating)).astype(jnp.bfloat16)
        return jnp.dot(hidden, down_weight, preferred_element_type=jnp.float32).astype(jnp.bfloat16)

    pieces = jnp.split(normed_two, 2 if rows % 32 == 0 else 1)
    arrived = [
        [passed_along(piece, "tok", d) for piece in pieces] for d in range(1, toks)
    ]
    total = middle + lax.optimization_barrier(feed(normed_two)).astype(jnp.float32)
    for d, blocks in enumerate(arrived, 1):
        back = [passed_along(feed(block), "tok", -d) for block in blocks]
        total = total + jnp.concatenate(back, 0).astype(jnp.float32)
    return total.astype(jnp.bfloat16).reshape(latents.shape)


def by_ring(
    latents,
    query_weight,
    key_weight,
    value_weight,
    output_weight,
    value_units,
    gate_units,
    down_weight,
):
    stream = latents.astype(jnp.float32)
    normed = normalize(stream).astype(jnp.bfloat16)
    joined = jnp.concatenate([query_weight, key_weight, value_weight], 1)
    projected = jnp.dot(
        lax.all_gather(normed, "tok", axis=0, tiled=True),
        joined,
        preferred_element_type=jnp.float32,
    ).astype(jnp.bfloat16)
    head_width = query_weight.shape[1]
    queries = projected[..., :head_width]
    key_part = projected[..., head_width : 2 * head_width]
    value_part = projected[..., 2 * head_width :]
    length_all, local_views, objects = (queries.shape[0], queries.shape[1], queries.shape[2])
    head_count = head_width // HS
    query_rows = length_all * local_views
    queries_flat = queries.reshape(query_rows, objects, head_count, HS)
    factor = HS ** (-0.5)

    def attend(states, key_block, value_block):
        key_rows = key_block.shape[0]

        def one_view(counter, inner):
            highest, totals, blended = inner
            key_view = lax.dynamic_index_in_dim(key_block, counter, 1, keepdims=False).reshape(
                key_rows, objects, head_count, HS
            )
            value_view = lax.dynamic_index_in_dim(value_block, counter, 1, keepdims=False).reshape(
                key_rows, objects, head_count, HS
            )
            scores = (
                jnp.einsum(
                    "ibhe,jbhe->bhij", queries_flat, key_view, preferred_element_type=jnp.float32
                )
                * factor
            )
            newest = jnp.maximum(highest, jnp.max(scores, -1))
            shrink = jnp.exp(highest - newest)
            weights = jnp.exp(scores - newest[..., None])
            totals = totals * shrink + jnp.sum(weights, -1)
            update = jnp.einsum(
                "bhij,jbhe->bhie",
                weights.astype(jnp.bfloat16),
                value_view,
                preferred_element_type=jnp.float32,
            )
            blended = blended * shrink[..., None] + update
            return (newest, totals, blended)

        return lax.fori_loop(0, key_block.shape[1], one_view, states)

    start_state = (
        jnp.full((objects, head_count, query_rows), -1e30, jnp.float32),
        jnp.zeros((objects, head_count, query_rows), jnp.float32),
        jnp.zeros((objects, head_count, query_rows, HS), jnp.float32),
    )
    stacked = jnp.stack([key_part, value_part])
    states = attend(start_state, key_part, value_part)

    def rotate(counter, bundle):
        inner, buffer_kv = bundle
        buffer_kv = passed_along(buffer_kv, "view", 1)
        return (attend(inner, buffer_kv[0], buffer_kv[1]), buffer_kv)

    states, stacked = lax.fori_loop(0, lax.axis_size("view") - 1, rotate, (states, stacked))
    highest, totals, blended = states
    attended = (blended / totals[..., None]).transpose(2, 0, 1, 3)
    attended = attended.reshape(length_all, local_views, objects, head_width).astype(jnp.bfloat16)
    full_output = lax.all_gather(output_weight, "tok", axis=0, tiled=True)
    own_rows = lax.all_to_all(attended, "tok", split_axis=0, concat_axis=3, tiled=True)
    groups = lax.axis_size("tok")
    grouped = own_rows.reshape(
        own_rows.shape[0], own_rows.shape[1], own_rows.shape[2], groups, head_width
    )
    weight_groups = full_output.reshape(groups, head_width, full_output.shape[1])
    group_parts = jnp.einsum(
        "rvbgc,gcd->rvbgd", grouped, weight_groups, preferred_element_type=jnp.float32
    ).astype(jnp.bfloat16)
    attention_out = jnp.sum(group_parts.astype(jnp.float32), 3)
    middle = stream + attention_out
    normed_two = normalize(middle).astype(jnp.bfloat16)
    gathered = lax.all_gather(normed_two, "tok", axis=0, tiled=True)
    linear = jnp.dot(gathered, value_units, preferred_element_type=jnp.float32)
    gating = jnp.dot(gathered, gate_units, preferred_element_type=jnp.float32)
    hidden = (linear * jax.nn.gelu(gating)).astype(jnp.bfloat16)
    feed_out = lax.psum_scatter(
        jnp.dot(hidden, down_weight, preferred_element_type=jnp.float32).astype(jnp.bfloat16),
        "tok",
        scatter_dimension=0,
        tiled=True,
    ).astype(jnp.float32)
    return (middle + feed_out).astype(jnp.bfloat16)


def on_device(latents, query_weight, *weights):
    head_count = query_weight.shape[1] // HS
    one_each = latents.shape[1] == 1 and latents.shape[2] == 1
    if one_each and head_count == lax.axis_size("view"):
        return by_heads(latents, query_weight, *weights)
    return by_ring(latents, query_weight, *weights)


def solution(mesh):
    return jax.shard_map(
        on_device,
        mesh=mesh,
        in_specs=(
            P("tok", "view", "obj", None),
            P(None, "tok"),
            P(None, "tok"),
            P(None, "tok"),
            P("tok", None),
            P(None, "tok"),
            P(None, "tok"),
            P("tok", None),
        ),
        out_specs=P("tok", "view", "obj", None),
        check_vma=False,
    )
```
